32 devices in a mesh: grp: 1 (over z), dz: 4 (over y), dy: 4 (over x), dx: 2 (over core).
Axes of the slice: x: 4, y: 4, z: 1, core: 2. Of those that a mesh axis runs over, the one named last changes fastest.
The devices are a block of a 4x4x8 slice.
Arguments:
- x_in: bfloat16 [8192, 4096], P(('grp', 'dx', 'dz'), 'dy')
- w_gate: bfloat16 [4096, 14336], P('dy', ('dz', 'dx'))
- w_up: bfloat16 [4096, 14336], P('dy', ('dz', 'dx'))
- w_down: bfloat16 [14336, 4096], P('dz', ('dy', 'dx'))
Outputs:
- output: bfloat16 [8192, 4096], P(('grp', 'dx', 'dz'), 'dy')
All inputs are finite; a program needn't handle non-finite values.
Results may differ from the reference program's by a relative error of at most 0.0124713.
Values are sent between devices in bfloat16 or wider.
A program may use at most 768 MiB of HBM per device.

```python
import jax
import jax.numpy as jnp
from jax import lax

N_ROWS = 8192
D_MODEL = 4096
D_FF = 14336
ROW_TILE = 1024


def setup_inputs(seed: int = 0, part: int = 0) -> dict:
    base_key = jax.random.key(seed)
    key_x = jax.random.fold_in(jax.random.fold_in(base_key, 1), part)
    key_gate = jax.random.fold_in(base_key, 2)
    key_up = jax.random.fold_in(base_key, 3)
    key_down = jax.random.fold_in(base_key, 4)
    x_in = jax.random.normal(key_x, (N_ROWS, D_MODEL), jnp.float32).astype(jnp.bfloat16)
    w_gate = (jax.random.normal(key_gate, (D_MODEL, D_FF), jnp.float32) * D_MODEL ** -0.5).astype(jnp.bfloat16)
    w_up = (jax.random.normal(key_up, (D_MODEL, D_FF), jnp.float32) * D_MODEL ** -0.5).astype(jnp.bfloat16)
    w_down = (jax.random.normal(key_down, (D_FF, D_MODEL), jnp.float32) * D_FF ** -0.5).astype(jnp.bfloat16)
    return {"x_in": x_in, "w_gate": w_gate, "w_up": w_up, "w_down": w_down}


def reference(x_in, w_gate, w_up, w_down):
    def row_tile(x_tile):
        gate_val = jnp.dot(x_tile, w_gate, preferred_element_type=jnp.float32).astype(jnp.bfloat16)
        up_val = jnp.dot(x_tile, w_up, preferred_element_type=jnp.float32).astype(jnp.bfloat16)
        hidden = (jax.nn.silu(gate_val.astype(jnp.float32)) * up_val.astype(jnp.float32)).astype(jnp.bfloat16)
        return jnp.dot(hidden, w_down, preferred_element_type=jnp.float32).astype(jnp.bfloat16)
    x_tiles = x_in.reshape(N_ROWS // ROW_TILE, ROW_TILE, D_MODEL)
    return lax.map(row_tile, x_tiles).reshape(N_ROWS, D_MODEL)
```

```python
import jax
import jax.numpy as jnp
from jax import lax
from jax.sharding import PartitionSpec as P


def solution(mesh):
    x_spec = P(("grp", "dx", "dz"), "dy")
    w_in_spec = P("dy", ("dz", "dx"))
    w_out_spec = P("dz", ("dy", "dx"))
    n_dx, n_dy, n_dz = mesh.shape["dx"], mesh.shape["dy"], mesh.shape["dz"]
    assert n_dx == 2

    def shift(a, axis, n, by):
        return lax.ppermute(a, axis, [(i, (i + by) % n) for i in range(n)])

    def ring_blocks(a, axis, n):
        blocks = [(0, a)]
        up = down = a
        for s in range(1, (n - 1) // 2 + 1):
            up, down = lax.optimization_barrier((shift(up, axis, n, 1), shift(down, axis, n, -1)))
            blocks += [(-s, up), (s, down)]
        if n % 2 == 0:
            half = a.shape[0] // 2
            far = [shift(up[:half], axis, n, 1), shift(down[half:], axis, n, -1)]
            blocks.append((n // 2, jnp.concatenate(far, axis=0)))
        return blocks

    def placed(parts, axis, n):
        me = lax.axis_index(axis)
        rows, cols = parts[0][1].shape
        out = jnp.zeros((n * rows, cols), parts[0][1].dtype)
        for offset, part in parts:
            out = lax.dynamic_update_slice(out, part, (lax.rem(me + offset + n, n) * rows, 0))
        return out

    def dot(a, b):
        return jnp.dot(a, b, preferred_element_type=jnp.float32)

    def hidden_of(gate_sum, up_sum):
        gate_val = gate_sum.astype(jnp.float32)
        up_val = up_sum.astype(jnp.bfloat16).astype(jnp.float32)
        return (jax.nn.silu(gate_val) * up_val).astype(jnp.bfloat16)

    def local_mlp(x_blk, wg_blk, wu_blk, wd_blk):
        wg = lax.all_gather(wg_blk, "dy", axis=0, tiled=True)

        x_q = lax.all_to_all(x_blk, "dy", 0, 1, tiled=True)
        x_q, wu_blk = lax.optimization_barrier((x_q, wu_blk))
        wu = lax.all_gather(wu_blk, "dy", axis=0, tiled=True)
        x_own = placed(ring_blocks(x_q, "dz", n_dz), "dz", n_dz)
        x_oth = shift(x_own, "dx", n_dx, 1)

        core = lax.axis_index("dx")
        half = wd_blk.shape[0] // n_dx
        wd_keep = lax.dynamic_slice_in_dim(wd_blk, core * half, half, 0)
        wd_give = lax.dynamic_slice_in_dim(wd_blk, (1 - core) * half, half, 0)
        wd_got = shift(wd_give, "dx", n_dx, 1)
        wd_first = jnp.where(core == 0, wd_keep, wd_got)
        wd_second = jnp.where(core == 0, wd_got, wd_keep)
        wd_pair = jnp.concatenate([wd_first, wd_second], axis=1)

        g_own, g_oth = (dot(x, wg).astype(jnp.bfloat16) for x in (x_own, x_oth))
        wu, wd_pair, g_own, g_oth = lax.optimization_barrier((wu, wd_pair, g_own, g_oth))
        wd_blocks = ring_blocks(wd_pair, "dy", n_dy)
        h_oth = hidden_of(g_oth, dot(x_oth, wu))
        h_own = hidden_of(g_own, dot(x_own, wu))

        outs, sums = [], []
        for i in range(len(wd_blocks)):
            if i == len(wd_blocks) - 2:
                tied = lax.optimization_barrier((h_own, h_oth, wd_blocks[-1][1]))
                h_own, h_oth, wd_blocks[-1] = tied[0], tied[1], (wd_blocks[-1][0], tied[2])
            wd = wd_blocks[i][1]
            part = dot(h_own, wd) + shift(dot(h_oth, wd), "dx", n_dx, 1)
            part, h_own, h_oth = lax.optimization_barrier((part, h_own, h_oth))
            if len(sums) >= 2:
                part, sums[-2] = lax.optimization_barrier((part, sums[-2]))
            sums.append(lax.psum_scatter(part, "dz", scatter_dimension=0, tiled=True))
        for (offset, _), out_sum in zip(wd_blocks, sums):
            done = out_sum.astype(jnp.bfloat16)
            outs.append((-offset, shift(done, "dy", n_dy, offset) if offset else done))
        return placed(outs, "dy", n_dy)

    return jax.shard_map(local_mlp, mesh=mesh, in_specs=(x_spec, w_in_spec, w_in_spec, w_out_spec), out_specs=x_spec, check_vma=False)
```
